32 devices in a mesh: space: 8 (over y, x, core), level: 4 (over z).
Axes of the slice: x: 2, y: 2, z: 4, core: 2. Of those that a mesh axis runs over, the one named last changes fastest.
Arguments:
- levels_in: bfloat16 [12, 48, 384, 512], P('level', 'space'), may hold values from -6 to 6
- kv_gain: float32 [512], replicated, may hold values from 0.25 to 1.75
- level_embed: float32 [12, 512], P('level'), may hold values from -3 to 3
- latent_queries: float32 [3, 512], replicated, may hold values from -6 to 6
- q_weight: bfloat16 [512, 512], replicated, may hold values from -0.25 to 0.25
- k_weight: bfloat16 [512, 512], replicated, may hold values from -0.25 to 0.25
- v_weight: bfloat16 [512, 512], replicated, may hold values from -0.25 to 0.25
- out_weight: bfloat16 [512, 512], replicated, may hold values from -0.25 to 0.25
- perc_scale: float32 [8], replicated, may hold values from 4 to 24
- attn_gain: float32 [512], replicated, may hold values from 0.25 to 1.75
- qkv_weight: bfloat16 [512, 1536], replicated, may hold values from -0.25 to 0.25
- swin_scale: float32 [8], replicated, may hold values from 4 to 24
- proj_weight: bfloat16 [512, 512], replicated, may hold values from -0.25 to 0.25
- mlp_gain: float32 [512], replicated, may hold values from 0.25 to 1.75
- up_weight: bfloat16 [512, 2048], replicated, may hold values from -0.25 to 0.25
- down_weight: bfloat16 [2048, 512], replicated, may hold values from -0.125 to 0.125
Outputs:
- latent_out: bfloat16 [3, 48, 384, 512], P(None, 'space', 'level')
The draws below stay inside these ranges and needn't reach their ends.
All inputs are finite; a program needn't handle non-finite values.
Results may differ from the reference program's by a relative error of at most 0.017.
Values may be sent and summed in bfloat16 or wider, within the bound.
A program may use at most 128 MiB of HBM per device.

```python
import math
import jax
import jax.numpy as jnp
from jax import lax

D = 512
HEADS = 8
MLP = 2048
LEVELS = 12
LATENT = 3
WR = 6
WC = 12
HEAD_DIM = 64
SR = 3
SC = 6
ROWS = 48
COLS = 384


def steps_of(key, dims, cuts, low, high):
    factor_of = 1.0
    for dim, blocks in cuts:
        steps = jax.random.uniform(jax.random.fold_in(jax.random.fold_in(key, 6), dim), (blocks,), jnp.float32, low / len(cuts), high / len(cuts))
        factor_of = factor_of * jnp.repeat(jnp.exp(steps), dims[dim] // blocks).reshape((-1,) + (1,) * (len(dims) - 1 - dim))
    return factor_of


def bell_draw(rng, dims, scale, bound, cuts=(), kind=jnp.bfloat16):
    values = jax.random.normal(rng, dims, jnp.float32) * scale
    if len(cuts) > 0:
        values = steps_of(rng, dims, cuts, -0.22, 0.18) * values
    return jnp.clip(values, min=-bound, max=bound).astype(kind)


def setup_inputs(seed: int = 0) -> dict:
    key_list = jax.random.split(jax.random.key(seed), 17)
    return {
        "levels_in": bell_draw(key_list[0], (LEVELS, ROWS, COLS, D), 1.0, 6.0, ((0, 4), (1, 8))),
        "kv_gain": jnp.clip(1.0 + 0.15 * jax.random.normal(key_list[1], (D,), jnp.float32), 0.25, 1.75),
        "level_embed": bell_draw(key_list[2], (LEVELS, D), 0.5, 3.0, ((0, 4),), jnp.float32),
        "latent_queries": bell_draw(key_list[3], (LATENT, D), 1.0, 6.0, (), jnp.float32),
        "q_weight": bell_draw(key_list[4], (D, D), D ** -0.5, 0.25),
        "k_weight": bell_draw(key_list[5], (D, D), D ** -0.5, 0.25),
        "v_weight": bell_draw(key_list[6], (D, D), D ** -0.5, 0.25),
        "out_weight": bell_draw(key_list[7], (D, D), D ** -0.5, 0.25),
        "perc_scale": jnp.clip(jnp.exp(jax.random.uniform(key_list[8], (HEADS,), jnp.float32, math.log(4.0), math.log(24.0))), 4.0, 24.0),
        "attn_gain": jnp.clip(1.0 + 0.15 * jax.random.normal(key_list[9], (D,), jnp.float32), 0.25, 1.75),
        "qkv_weight": bell_draw(key_list[10], (D, 3 * D), D ** -0.5, 0.25),
        "swin_scale": jnp.clip(jnp.exp(jax.random.uniform(key_list[11], (HEADS,), jnp.float32, math.log(4.0), math.log(24.0))), 4.0, 24.0),
        "proj_weight": bell_draw(key_list[12], (D, D), D ** -0.5, 0.25),
        "mlp_gain": jnp.clip(1.0 + 0.15 * jax.random.normal(key_list[13], (D,), jnp.float32), 0.25, 1.75),
        "up_weight": bell_draw(key_list[14], (D, MLP), D ** -0.5, 0.25),
        "down_weight": bell_draw(key_list[15], (MLP, D), MLP ** -0.5, 0.125),
    }


def layer_norm(values, gain):
    center = values - lax.optimization_barrier(jnp.mean(values, -1, keepdims=True))
    spread = lax.optimization_barrier(jnp.mean(center * center, -1, keepdims=True))
    return center * lax.rsqrt(spread + 1e-05) * gain

def unit_heads(values):
    return values * lax.rsqrt(lax.optimization_barrier(jnp.mean(values * values, -1, keepdims=True)) + 1e-06)

def perceiver_pool(tokens, query_unit, k_weight, v_weight, perc_scale):
    levels, rows, cols, width = tokens.shape
    heads = query_unit.shape[1]
    head_dim = width // heads
    keys = jnp.dot(tokens, k_weight, preferred_element_type=jnp.float32).astype(jnp.bfloat16)
    values = jnp.dot(tokens, v_weight, preferred_element_type=jnp.float32).astype(jnp.bfloat16)
    key_unit = unit_heads(keys.astype(jnp.float32).reshape(levels, rows, cols, heads, head_dim))
    scores = jnp.einsum('ahd,lrchd->alrch', query_unit, key_unit, precision=lax.Precision.HIGHEST)
    scores = scores * (perc_scale / head_dim)
    weights = jnp.exp(scores)
    denom = lax.optimization_barrier(jnp.sum(weights, axis=1))
    split_values = values.reshape(levels, rows, cols, heads, head_dim).astype(jnp.float32)
    weights_low = weights.astype(jnp.bfloat16).astype(jnp.float32)
    numer = jnp.einsum('alrch,lrchd->archd', weights_low, split_values, precision=lax.Precision.HIGHEST)
    pooled = numer / denom[..., None]
    return pooled.reshape(pooled.shape[0], rows, cols, width).astype(jnp.bfloat16)

def swin_block(block, first_row, total_rows, attn_gain, qkv_weight, swin_scale, proj_weight, mlp_gain, up_weight, down_weight):
    latent_count, rows, cols, width = block.shape
    heads = swin_scale.shape[0]
    head_dim = width // heads
    window_count = cols // WC
    tokens_per = latent_count * rows * WC
    normed = layer_norm(block.astype(jnp.float32), attn_gain).astype(jnp.bfloat16)
    packed = jnp.dot(normed, qkv_weight, preferred_element_type=jnp.float32).astype(jnp.bfloat16)
    windows = packed.reshape(latent_count, rows, window_count, WC, 3 * width).transpose(2, 0, 1, 3, 4)
    windows = windows.reshape(window_count, tokens_per, 3, heads, head_dim)
    query_part = unit_heads(windows[:, :, 0].astype(jnp.float32))
    key_part = unit_heads(windows[:, :, 1].astype(jnp.float32))
    value_part = windows[:, :, 2].astype(jnp.float32)
    scores = jnp.einsum('wihd,wjhd->whij', query_part, key_part, precision=lax.Precision.HIGHEST)
    scores = scores * (swin_scale / head_dim)[:, None, None]
    position = jnp.arange(tokens_per, dtype=jnp.int32) // WC % rows + first_row
    region = (position >= total_rows - WR).astype(jnp.int32) + (position >= total_rows - SR).astype(jnp.int32)
    allowed = region[:, None] == region[None, :]
    weights = jnp.where(allowed, jnp.exp(scores), jnp.float32(0.0))
    probs = (weights / lax.optimization_barrier(jnp.sum(weights, -1, keepdims=True))).astype(jnp.bfloat16)
    mixed = jnp.einsum('whij,wjhd->wihd', probs.astype(jnp.float32), value_part, precision=lax.Precision.HIGHEST)
    mixed = mixed.astype(jnp.bfloat16).reshape(window_count, latent_count, rows, WC, width)
    mixed = mixed.transpose(1, 2, 0, 3, 4).reshape(latent_count, rows, cols, width)
    branch = jnp.dot(mixed, proj_weight, preferred_element_type=jnp.float32).astype(jnp.bfloat16)
    middle = block.astype(jnp.float32) + branch.astype(jnp.float32)
    mlp_in = layer_norm(middle, mlp_gain).astype(jnp.bfloat16)
    hidden = jax.nn.gelu(jnp.dot(mlp_in, up_weight, preferred_element_type=jnp.float32)).astype(jnp.bfloat16)
    final = middle + jnp.dot(hidden, down_weight, preferred_element_type=jnp.float32)
    return final.astype(jnp.bfloat16)

def reference(levels_in, kv_gain, level_embed, latent_queries, q_weight, k_weight, v_weight, out_weight, perc_scale, attn_gain, qkv_weight, swin_scale, proj_weight, mlp_gain, up_weight, down_weight):
    queries = jnp.dot(latent_queries.astype(jnp.bfloat16), q_weight, preferred_element_type=jnp.float32)
    query_unit = unit_heads(queries.reshape(LATENT, HEADS, HEAD_DIM))
    block_count = ROWS // WR

    def encode(index):
        start = (index * WR).astype(jnp.int32)
        raw = lax.dynamic_slice_in_dim(levels_in, start, WR, 1)
        tokens = (layer_norm(raw.astype(jnp.float32), kv_gain) + level_embed[:, None, None, :]).astype(jnp.bfloat16)
        pooled = perceiver_pool(tokens, query_unit, k_weight, v_weight, perc_scale)
        latent = latent_queries[:, None, None, :] + jnp.dot(pooled, out_weight, preferred_element_type=jnp.float32)
        return latent.astype(jnp.bfloat16)
    blocks = lax.map(encode, jnp.arange(block_count, dtype=jnp.int32))
    latent = blocks.transpose(1, 0, 2, 3, 4).reshape(LATENT, ROWS, COLS, D)
    rolled = jnp.roll(latent, (-SR, -SC), axis=(1, 2))

    def layer(index):
        start = (index * WR).astype(jnp.int32)
        block = lax.dynamic_slice_in_dim(rolled, start, WR, 1)
        return swin_block(block, start, ROWS, attn_gain, qkv_weight, swin_scale, proj_weight, mlp_gain, up_weight, down_weight)
    finals = lax.map(layer, jnp.arange(block_count, dtype=jnp.int32))
    final = finals.transpose(1, 0, 2, 3, 4).reshape(LATENT, ROWS, COLS, D)
    return jnp.roll(final, (SR, SC), axis=(1, 2))
```

```python
import jax
import jax.numpy as jnp
from jax import lax
from jax.experimental import pallas as pl
from jax.sharding import PartitionSpec as P


WR = 6
WC = 12
SR = 3
SC = 6
LANES = 128
BF = jnp.bfloat16
F32 = jnp.float32


def from_behind(block, axis, distance):
    count = lax.axis_size(axis)
    route = [((i - distance) % count, i) for i in range(count)]
    return lax.ppermute(block, axis, route)


def dot(a, b):
    return jnp.dot(a, b, preferred_element_type=F32)


def layer_norm(values, gain):
    center = values - jnp.mean(values, -1, keepdims=True)
    spread = jnp.mean(center * center, -1, keepdims=True)
    return center * lax.rsqrt(spread + 1e-05) * gain


def partial_kernel(x_ref, gain_ref, embed_ref, k_ref, v_ref, q_ref, ones_ref, spread_ref, out_ref):
    levels, tokens, width = x_ref.shape[1:]
    latents = out_ref.shape[1] // tokens
    head_dim = width // 8
    x = x_ref[0].astype(F32)
    normed = layer_norm(x, gain_ref[...][None]) + embed_ref[...]
    normed = normed.astype(BF).reshape(levels * tokens, width)
    keys = dot(normed, k_ref[...]).astype(BF)
    values = dot(normed, v_ref[...]).astype(BF).astype(F32)
    keys32 = keys.astype(F32)
    squares = dot((keys32 * keys32).astype(BF), ones_ref[...])
    raw = dot(keys, q_ref[...])
    raw = raw[:, :LANES] + raw[:, LANES:]
    weights = jnp.exp(raw * lax.rsqrt(squares * (1.0 / head_dim) + 1e-06))
    denom = weights[:tokens]
    for l in range(1, levels):
        denom = denom + weights[l * tokens : (l + 1) * tokens]
    low = weights.astype(BF)
    for a in range(latents):
        wide = dot(low, spread_ref[:, a * width : (a + 1) * width]) * values
        numer = wide[:tokens]
        for l in range(1, levels):
            numer = numer + wide[l * tokens : (l + 1) * tokens]
        out_ref[0, a * tokens : (a + 1) * tokens, :] = numer.astype(BF)
    pad = 2 * LANES - tokens
    turned = jnp.concatenate([denom, jnp.ones((pad, LANES), F32)], 0).T
    halves = []
    for t in range(2):
        parts = [
            turned[a * 8 : a * 8 + 8, t * LANES : (t + 1) * LANES] for a in range(latents)
        ]
        parts.append(jnp.ones((8, width - latents * LANES), F32))
        halves.append(jnp.concatenate(parts, 1))
    out_ref[0, latents * tokens :, :] = jnp.concatenate(halves, 0).astype(BF)


def latent_kernel(sum_ref, lq_ref, out_w_ref, spread_ref, head_ref, tail_ref):
    latents, half, _ = head_ref.shape
    tokens = 2 * half
    turned = sum_ref[latents * tokens :, :].astype(F32).T.astype(BF)
    first = spread_ref[0]
    second = spread_ref[1]
    for a in range(latents):
        block = turned[a * LANES : (a + 1) * LANES]
        denom = jnp.concatenate([dot(block, first), dot(block, second)[: tokens - LANES]], 0)
        numer = sum_ref[a * tokens : (a + 1) * tokens, :].astype(F32)
        pooled = (numer / denom).astype(BF)
        latent = lq_ref[a : a + 1, :] + dot(pooled, out_w_ref[...])
        head_ref[a] = latent[:half].astype(BF)
        tail_ref[a] = latent[half:].astype(BF)


def swin_kernel(
    tail_ref,
    ahead_ref,
    mask_ref,
    attn_gain_ref,
    qkv_ref,
    scale_ref,
    ones_ref,
    ones_t_ref,
    proj_ref,
    mlp_gain_ref,
    up_ref,
    down_ref,
    own_ref,
    back_ref,
):
    latents, half, width = tail_ref.shape
    heads = 8
    head_dim = width // heads
    side = latents * half
    block = jnp.concatenate(
        [
            tail_ref[...].astype(F32).reshape(side, width),
            ahead_ref[...].astype(F32).reshape(side, width),
        ],
        0,
    )
    normed = layer_norm(block, attn_gain_ref[...]).astype(BF)
    packed = dot(normed, qkv_ref[...]).astype(BF)
    q = packed[:, :width]
    k = packed[:, width : 2 * width]
    v = packed[:, 2 * width :]
    q32 = q.astype(F32)
    k32 = k.astype(F32)
    q_norm = dot((q32 * q32).astype(BF), ones_ref[...])
    q_norm = lax.rsqrt(q_norm * (1.0 / head_dim) + 1e-06) * scale_ref[...]
    k_norm = lax.dot_general(
        ones_t_ref[...],
        (k32 * k32).astype(BF),
        (((1,), (1,)), ((), ())),
        preferred_element_type=F32,
    )
    k_norm = lax.rsqrt(k_norm * (1.0 / head_dim) + 1e-06)
    mask = mask_ref[...]
    mixed = []
    for h in range(heads):
        cut = slice(h * head_dim, (h + 1) * head_dim)
        scores = lax.dot_general(
            q[:, cut], k[:, cut], (((1,), (1,)), ((), ())), preferred_element_type=F32
        )
        scores = scores * q_norm[:, h : h + 1] * k_norm[h : h + 1, :]
        weights = jnp.exp(scores) * mask
        total = jnp.sum(weights, -1, keepdims=True)
        mixed.append(dot(weights.astype(BF), v[:, cut]) / total)
    mixed = jnp.concatenate(mixed, 1).astype(BF)
    branch = dot(mixed, proj_ref[...]).astype(BF)
    middle = block + branch.astype(F32)
    mlp_in = layer_norm(middle, mlp_gain_ref[...]).astype(BF)
    hidden = jax.nn.gelu(dot(mlp_in, up_ref[...])).astype(BF)
    final = middle + dot(hidden, down_ref[...])
    own_ref[...] = final[:side].reshape(latents, half, width).astype(BF)
    back_ref[...] = final[side:].reshape(latents, half, width).astype(BF)


def whole(shape):
    return pl.BlockSpec(shape, lambda *_: (0,) * len(shape))


def shards(
    levels_in,
    kv_gain,
    level_embed,
    latent_queries,
    q_weight,
    k_weight,
    v_weight,
    out_weight,
    perc_scale,
    attn_gain,
    qkv_weight,
    swin_scale,
    proj_weight,
    mlp_gain,
    up_weight,
    down_weight,
):
    levels, rows, all_cols, width = levels_in.shape
    latents = latent_queries.shape[0]
    heads = perc_scale.shape[0]
    head_dim = width // heads
    mlp = up_weight.shape[1]
    owners = lax.axis_size("level")
    cols = all_cols // owners
    step = 2 * WC
    chunks = cols // step
    tokens = rows * step
    half = SR * step
    packed_rows = latents * tokens + 16
    assert rows == WR and heads == 8 and LANES < tokens <= 2 * LANES

    queries = dot(latent_queries.astype(BF), q_weight).reshape(latents, heads, head_dim)
    unit = queries * lax.rsqrt(jnp.mean(queries * queries, -1, keepdims=True) + 1e-06)
    unit = unit * (perc_scale / head_dim)[None, :, None]
    lane_head = jnp.arange(width) // head_dim
    col = jnp.arange(LANES)
    used = col < latents * heads
    same = (lane_head[:, None] == (col % heads)[None, :]) & used[None, :]
    unit_t = unit.reshape(latents, width).T
    spread_q = jnp.repeat(unit_t, heads, axis=1)
    spread_q = jnp.pad(spread_q, ((0, 0), (0, LANES - latents * heads)))
    spread_q = jnp.where(same, spread_q, 0.0)
    q_high = spread_q.astype(BF)
    q_low = (spread_q - q_high.astype(F32)).astype(BF)
    q_mat = jnp.concatenate([q_high, q_low], 1)
    ones = same.astype(BF)
    wide_lane = jnp.arange(latents * width)
    wide_col = wide_lane // width * heads + wide_lane % width // head_dim
    spread = (col[:, None] == wide_col[None, :]).astype(BF)
    row16 = jnp.arange(16)
    den_spread = jnp.stack(
        [(row16[:, None] - t * heads == lane_head[None, :]) for t in range(2)]
    ).astype(BF)
    ones_t = (row16[:, None] == lane_head[None, :]).astype(BF)
    scale_row = jnp.pad(swin_scale / head_dim, (0, LANES - heads))[None]

    place = jnp.arange(2 * latents * half)
    side = place // (latents * half)
    window = place % step // WC
    last = lax.axis_index("space") == lax.axis_size("space") - 1
    mask = (window[:, None] == window[None, :]) & (
        (side[:, None] == side[None, :]) | jnp.logical_not(last)
    )
    mask = mask.astype(F32)

    partial = pl.pallas_call(
        partial_kernel,
        grid=(owners,),
        in_specs=[
            pl.BlockSpec((1, levels, tokens, width), lambda i: (i, 0, 0, 0)),
            whole((1, width)),
            whole((levels, 1, width)),
            whole((width, width)),
            whole((width, width)),
            whole((width, 2 * LANES)),
            whole((width, LANES)),
            whole((LANES, latents * width)),
        ],
        out_specs=pl.BlockSpec((1, packed_rows, width), lambda i: (i, 0, 0)),
        out_shape=jax.ShapeDtypeStruct((owners, packed_rows, width), BF),
        cost_estimate=pl.CostEstimate(
            flops=owners * levels * tokens * width * width * 8,
            bytes_accessed=12_000_000,
            transcendentals=0,
        ),
        name="partials",
    )
    latent_of = pl.pallas_call(
        latent_kernel,
        out_shape=[jax.ShapeDtypeStruct((latents, half, width), BF)] * 2,
        cost_estimate=pl.CostEstimate(
            flops=latents * tokens * width * width * 8,
            bytes_accessed=3_000_000,
            transcendentals=0,
        ),
        name="latents",
    )
    layer = pl.pallas_call(
        swin_kernel,
        out_shape=[jax.ShapeDtypeStruct((latents, half, width), BF)] * 2,
        cost_estimate=pl.CostEstimate(
            flops=latents * tokens * width * (4 * width + 2 * mlp) * 4,
            bytes_accessed=10_000_000,
            transcendentals=0,
        ),
        name="layer",
    )

    def piece(chunk):
        parts = []
        for q in range(owners):
            start = q * cols + SC + chunk * step
            stop = start + step
            if stop <= all_cols:
                part = levels_in[:, :, start:stop]
            else:
                part = jnp.concatenate(
                    [levels_in[:, :, start:], levels_in[:, :, : stop - all_cols]], 2
                )
            parts.append(part.reshape(levels, tokens, width))
        return jnp.stack(parts)

    order = [chunks - 1] + list(range(chunks - 1))
    sums = {}
    for chunk in order:
        sent = partial(
            piece(chunk),
            kv_gain[None],
            level_embed[:, None, :],
            k_weight,
            v_weight,
            q_mat,
            ones,
            spread,
        )
        sums[chunk] = lax.psum_scatter(
            sent.reshape(owners * packed_rows, width), "level", scatter_dimension=0, tiled=True
        )
    done = {}
    for chunk in order:
        head, tail = latent_of(sums[chunk], latent_queries, out_weight, den_spread)
        ahead = from_behind(head, "space", -1)
        own, back = layer(
            tail,
            ahead,
            mask,
            attn_gain[None],
            qkv_weight,
            scale_row,
            ones,
            ones_t,
            proj_weight,
            mlp_gain[None],
            up_weight,
            down_weight,
        )
        top = from_behind(back, "space", 1)
        done[chunk] = jnp.concatenate(
            [
                top.reshape(latents, SR, step, width),
                own.reshape(latents, SR, step, width),
            ],
            1,
        )
    edge = done[chunks - 1]
    first = from_behind(edge[:, :, step - SC :], "level", 1)
    pieces = [first] + [done[c] for c in range(chunks - 1)] + [edge[:, :, : step - SC]]
    return jnp.concatenate(pieces, 2)


def solution(mesh):
    placed = (P("level", "space", None, None), P(), P("level", None)) + (P(),) * 13
    return jax.shard_map(
        shards,
        mesh=mesh,
        in_specs=placed,
        out_specs=P(None, "space", "level", None),
        check_vma=False,
    )
```
